32 devices in a mesh: ga: 8 (over z, x), ta: 4 (over y, core).
Axes of the slice: x: 2, y: 2, z: 4, core: 2. Of those that a mesh axis runs over, the one named last changes fastest.
Arguments:
- density: bfloat16 [2, 6144, 16384], P(None, 'ga', 'ta'), may hold values from -6 to 6
- coulomb: float32 [6144], P('ga'), may hold values from 0.001275776 to 0.01275776
- row_block: int32 [1], replicated, may hold values from 0 to 67
Outputs:
- kernel: float32 [4, 4096, 2, 240], P('ta', 'ga')
The draws below stay inside these ranges and needn't reach their ends.
Inputs may be any that keep to these rules, and one draw needn't show every extreme that they name: The rows row_block * 240 to row_block * 240 + 239 lie among the 16384 transitions.
All inputs are finite; a program needn't handle non-finite values.
Results may differ from the reference program's by a relative error of at most 0.0025.
Values may be sent and summed in bfloat16 or wider, within the bound.
A program may use at most 64 MiB of HBM per device.

```python
import math
import jax
import jax.numpy as jnp
from jax import lax

NG = 6144
NC = 16384
RB = 240
N_TA = 4


def shard_levels(key, dims, shards, least, high):
    gain, own = 1.0, jax.random.fold_in(key, 6)
    for position, shards_of in shards:
        steps = jnp.exp(jax.random.uniform(jax.random.fold_in(own, position), (shards_of,), jnp.float32, least / len(shards), high / len(shards)))
        gain = gain * jnp.repeat(steps, dims[position] // shards_of).reshape([-1 if axis == position else 1 for axis in range(len(dims))])
    return gain


def gaussian(stream_key, shape, scale, most, split=(), held_as=jnp.bfloat16):
    drawn = jax.random.normal(stream_key, shape, jnp.float32) * scale
    if len(split) > 0:
        drawn = shard_levels(stream_key, shape, split, -0.22, 0.18) * drawn
    return jnp.clip(drawn, min=-most, max=most).astype(held_as)


def setup_inputs(seed: int = 0) -> dict:
    key_list = jax.random.split(jax.random.key(seed), 4)
    density = gaussian(key_list[0], (2, NG, NC), 1.0, 6.0, ((1, 8), (2, 4)))
    coulomb = jnp.clip(jnp.exp(math.log(0.01275776) - 2.3025851 * jax.random.uniform(key_list[1], (NG,), jnp.float32) ** shard_levels(key_list[1], (NG,), ((0, 8),), -0.2, 0.2)), 0.001275776, 0.01275776)
    row_block = jax.random.randint(key_list[2], (1,), 0, NC // RB).astype(jnp.int32)
    return dict(density=density, coulomb=coulomb, row_block=row_block)


def stack_left(folded):
    real_part = folded[0]
    imag_part = folded[1]
    upper_half = jnp.concatenate([real_part, -imag_part], axis=1)
    lower_half = jnp.concatenate([imag_part, real_part], axis=1)
    return jnp.concatenate([upper_half, lower_half], axis=0)


def reference(density, coulomb, row_block):
    offset = (row_block[0] * RB).astype(jnp.int32)
    picked = lax.dynamic_slice_in_dim(density, offset, RB, 2)
    folded = (coulomb[None, :, None] * picked.astype(jnp.float32)).astype(jnp.bfloat16)
    stacked = stack_left(folded)
    flattened = density.reshape(2 * NG, NC)
    kernel = lax.dot_general(flattened, stacked, (((0,), (0,)), ((), ())), preferred_element_type=jnp.float32)
    return kernel.reshape(N_TA, NC // N_TA, 2, RB)
```

```python
import functools

import jax
import jax.numpy as jnp
from jax import lax
from jax.experimental import pallas as pl
from jax.experimental.pallas import tpu as pltpu
from jax.sharding import PartitionSpec as P

RB = 240
LANES = 128
UNITS = ((16, "A"), (16, "C"), (32, "A"), (32, "C"), (64, "A"), (48, "A"), (24, "A"), (8, "A"))
STEPS = (
    ("e1", 0, 0), ("e2", 0, 0), ("e1", 1, 0), ("s", 0, 0), ("s", 0, 1), ("s", 0, 2), ("e2", 1, 0), ("e1", 2, 0),
    ("s", 1, 0), ("s", 1, 1), ("e1", 3, 0), ("s", 1, 2), ("e2", 2, 0), ("s", 2, 0), ("s", 2, 1), ("e2", 3, 0),
    ("s", 3, 0), ("e1", 4, 0), ("s", 3, 1), ("s", 2, 2), ("s", 3, 2), ("e1", 5, 0), ("e2", 4, 0), ("s", 4, 0),
    ("e1", 6, 0), ("e1", 7, 0), ("s", 4, 1), ("e2", 5, 0), ("s", 1, 3), ("e2", 6, 0), ("e2", 7, 0), ("s", 4, 2),
    ("s", 3, 3), ("k", 0, 0), ("t", 0, 0), ("s", 5, 0), ("k", 0, 1), ("t", 0, 1), ("k", 0, 2), ("k", 0, 3),
    ("k", 1, 0), ("t", 1, 0), ("k", 1, 1), ("t", 1, 1), ("k", 1, 2), ("k", 1, 3), ("s", 5, 1), ("k", 2, 0),
    ("t", 2, 0), ("k", 2, 1), ("t", 2, 1), ("t2", 0, 0), ("k", 2, 2), ("k", 2, 3), ("s", 5, 2), ("k", 3, 0),
    ("t", 3, 0), ("k", 3, 1), ("t", 3, 1), ("k", 3, 2), ("k", 3, 3), ("k", 4, 0), ("t", 4, 0), ("t2", 2, 0),
    ("k", 4, 1), ("t", 4, 1), ("k", 4, 2), ("k", 4, 3), ("k", 5, 0), ("k", 5, 1), ("s", 6, 0), ("k", 5, 2),
    ("s", 6, 1), ("t", 5, 0), ("k", 5, 3), ("t2", 1, 0), ("k", 6, 0), ("s", 6, 2), ("k", 6, 1), ("s", 7, 0),
    ("t2", 4, 0), ("s", 7, 1), ("s", 7, 2), ("k", 6, 2), ("t", 5, 1), ("k", 6, 3), ("k", 7, 0), ("k", 7, 1),
    ("k", 7, 2), ("k", 7, 3), ("s", 0, 3), ("s", 2, 3), ("s", 4, 3), ("s", 5, 3), ("t2", 3, 0), ("s", 6, 3),
    ("s", 7, 3), ("t2", 5, 0), ("t", 6, 0), ("t", 6, 1), ("t", 7, 0), ("t", 7, 1), ("t2", 6, 0), ("t2", 7, 0),
    ("f", 0, 0), ("f", 1, 0), ("f", 2, 0), ("f", 3, 0), ("f", 4, 0), ("f", 5, 0), ("f", 6, 0), ("f", 7, 0),
)
HOPS = {"A": (0, 1, 2), "B": (1, 2, 0), "C": (1, 0, 2), "D": (0, 2, 1)}
DIRECT = 1
MESH = pl.DeviceIdType.MESH
VMEM_BYTES = 50 * 2**20
PICK_BYTES = 53 * 2**20


def stack_left(folded):
    real_part = folded[0]
    imag_part = folded[1]
    upper_half = jnp.concatenate([real_part, -imag_part], axis=1)
    lower_half = jnp.concatenate([imag_part, real_part], axis=1)
    return jnp.concatenate([upper_half, lower_half], axis=0)


def plain_body(density, coulomb, row_block):
    local_g = density.shape[1]
    col_width = density.shape[2]
    group_index = lax.axis_index("ta")
    column = row_block[0] * RB + jnp.arange(RB, dtype=jnp.int32)
    owner_index = column // col_width
    position = jnp.clip(column - group_index * col_width, 0, col_width - 1)
    picked = jnp.take(density, position, axis=2)
    weighted = (coulomb[None, :, None] * picked.astype(jnp.float32)).astype(jnp.bfloat16)
    masked = jnp.where(
        (owner_index == group_index)[None, None, :], weighted.astype(jnp.float32), 0.0
    )
    folded = lax.psum(masked.astype(jnp.bfloat16), "ta")
    stacked = stack_left(folded)
    own_rows = col_width // lax.axis_size("ga")
    sliced = density.reshape(2 * local_g, lax.axis_size("ga") * own_rows)
    kernel = lax.psum_scatter(
        lax.dot_general(
            sliced, stacked, (((0,), (0,)), ((), ())), preferred_element_type=jnp.float32
        ),
        "ga",
        scatter_dimension=0,
        tiled=True,
    )
    return kernel.reshape(1, kernel.shape[0], 2, RB)


def pick_kernel(local_g, width, window, row_block, density, out, held, sems):
    first = row_block[0] * RB - lax.axis_index("ta") * width
    start = jnp.minimum(lax.div(jnp.maximum(first, 0), LANES) * LANES, width - window)
    start = pl.multiple_of(start, LANES)
    pieces = 2
    copies = []
    for piece in range(pieces):
        rows = pl.ds(piece * local_g, local_g)
        view = density.at[rows, pl.ds(start, window)]
        copies.append(pltpu.make_async_copy(view, held.at[rows], sems.at[piece]))
        copies[piece].start()
    row = lax.broadcasted_iota(jnp.int32, (RB, window), 0)
    column = lax.broadcasted_iota(jnp.int32, (RB, window), 1)
    chosen = jnp.where(start + column == first + row, 1.0, 0.0).astype(jnp.bfloat16)
    for piece in range(pieces):
        copies[piece].wait()
        part, first_g = divmod(piece * local_g, local_g)
        out[part, :, first_g : first_g + local_g] = lax.dot_general(
            chosen,
            held[piece * local_g : (piece + 1) * local_g, :],
            (((1,), (1,)), ((), ())),
            preferred_element_type=jnp.float32,
        ).astype(jnp.bfloat16)


def flipped(index, bits):
    for bit in bits:
        step = 2**bit
        index = index + step * (1 - 2 * lax.rem(lax.div(index, step), 2))
    return index


def exchange_kernel(
    n_ga, local_g, own,
    masked, coulomb, density, out,
    dens, core_half, half, far_half, full, lhs, acc, s0, r0, s1, r1,
    dens_sem, core_ss, core_rs, far_ss, far_rs, last_ss, last_rs, ss0, rs0, ss1, rs1,
    two_away, three_away,
):
    f32, bf16 = jnp.float32, jnp.bfloat16
    ga = lax.axis_index("ga")
    ta = lax.axis_index("ta")
    core = lax.rem(ta, 2)
    core_peer = {"ta": flipped(ta, (0,))}
    far_peer = {"ta": flipped(ta, (1,))}
    hop_peer = {bits: {"ga": flipped(ga, bits)} for bits in ((0,), (1,), (2,), (1, 2))}
    sizes = [rows for rows, _ in UNITS]
    kinds = [kind for _, kind in UNITS]
    offsets = [sum(sizes[:u]) for u in range(len(UNITS))]

    def load(r):
        block = flipped(ga, [bit for bit in range(3) if r >> bit & 1])
        column = pl.multiple_of(block * own, own)
        return pltpu.make_async_copy(density.at[:, pl.ds(column, own)], dens.at[r], dens_sem.at[r])

    inner = lax.rem(lax.div(lax.div(ga, 2) + 1, 2), 2)
    barrier = pltpu.get_barrier_semaphore()
    peers = [core_peer, far_peer, hop_peer[0,], hop_peer[1,]]

    def signal(semaphore, peer):
        pl.semaphore_signal(semaphore, inc=1, device_id=peer, device_id_type=MESH)

    for peer in peers:
        signal(barrier, peer)

    @pl.when(inner == 1)
    def _():
        signal(barrier, hop_peer[1, 2])

    for r in range(n_ga):
        load(n_ga - 1 - r).start()
    pl.semaphore_wait(barrier, len(peers) + inner)

    def tell_two():
        @pl.when(inner == 1)
        def _():
            signal(two_away, hop_peer[1,])
            signal(two_away, hop_peer[1, 2])

    def hear_two():
        pl.semaphore_wait(two_away, 1)

        @pl.when(inner == 1)
        def _():
            signal(three_away, hop_peer[1,])

    def hear_three():
        @pl.when(inner == 0)
        def _():
            pl.semaphore_wait(three_away, 1)

    def remote(src, dst, send, recv, peer):
        return pltpu.make_async_remote_copy(
            src_ref=src, dst_ref=dst, send_sem=send, recv_sem=recv,
            device_id=peer, device_id_type=MESH,
        )

    def rows_of(u):
        return pl.ds(offsets[u], sizes[u])

    def both(u):
        return pl.ds(2 * offsets[u], 2 * sizes[u])

    def to_core(u):
        view = rows_of(u)
        source, target = masked.at[1 - core, view], core_half.at[0, view]
        return remote(source, target, core_ss.at[u], core_rs.at[u], core_peer)

    def to_far(u):
        view = rows_of(u)
        if u < DIRECT:
            source, target = masked.at[:, view], far_half.at[:, view]
        else:
            source, target = half.at[view], far_half.at[0, view]
        return remote(source, target, far_ss.at[u], far_rs.at[u], far_peer)

    def to_last(u):
        view = rows_of(u)
        if u < DIRECT:
            source, target = full.at[:, view], core_half.at[:, view]
        else:
            source = target = full.at[core, view]
        return remote(source, target, last_ss.at[u], last_rs.at[u], core_peer)

    def from_last(u):
        view = full.at[1 - core, rows_of(u)]
        return to_last(u) if u < DIRECT else remote(view, view, last_ss.at[u], last_rs.at[u], core_peer)

    def send0(u, q):
        sem = 4 * u + q
        peer = hop_peer[HOPS[kinds[u]][:1]]
        return remote(s0.at[q, both(u)], r0.at[q, both(u)], ss0.at[sem], rs0.at[sem], peer)

    def send1(u, k):
        sem = 3 * u + k
        if kinds[u] == "D":
            bits = ((1, 2), (2,), (1,))[k]
        else:
            bits = HOPS[kinds[u]][2:] if k == 2 else HOPS[kinds[u]][1:2]
        return remote(s1.at[k, both(u)], r1.at[k, both(u)], ss1.at[sem], rs1.at[sem], hop_peer[bits])

    for u in range(len(UNITS)):
        if u < DIRECT:
            to_far(u).start()
        else:
            to_core(u).start()
    for u in range(DIRECT, len(UNITS)):
        rows = rows_of(u)
        to_core(u).wait_recv()
        half[rows] = (masked[core, rows].astype(f32) + core_half[0, rows].astype(f32)).astype(bf16)
        to_far(u).start()
    tell_two()

    waited = set()

    def product(u, q, sent):
        first, second, third = HOPS[kinds[u]]
        r = 2**second * (1 - q // 2) + 2**third * (1 - q % 2) + (2**first if sent else 0)
        if r not in waited:
            load(r).wait()
            waited.add(r)
        return jnp.dot(lhs[both(u)], dens[r], preferred_element_type=f32)

    def step(op, u, q):
        view = both(u)
        rows = rows_of(u)
        if op == "e1":
            to_far(u).wait_recv()
            if u < DIRECT:
                full[:, rows] = (masked[:, rows].astype(f32) + far_half[:, rows].astype(f32)).astype(bf16)
            else:
                full[core, rows] = (half[rows].astype(f32) + far_half[0, rows].astype(f32)).astype(bf16)
            to_last(u).start()
        elif op == "e2":
            from_last(u).wait_recv()
            picked = full[:, rows].astype(f32)
            if u < DIRECT:
                picked = picked + core_half[:, rows].astype(f32)
            both_parts = (coulomb[...][None, None, :] * picked).astype(bf16)
            upper = pl.ds(2 * offsets[u], sizes[u])
            lower = pl.ds(2 * offsets[u] + sizes[u], sizes[u])
            lhs[upper, 0:local_g] = both_parts[0]
            lhs[upper, local_g : 2 * local_g] = both_parts[1]
            lhs[lower, 0:local_g] = -both_parts[1]
            lhs[lower, local_g : 2 * local_g] = both_parts[0]
        elif op == "s":
            s0[q, view] = product(u, q, True).astype(bf16)
            send0(u, q).start()
        elif op == "k":
            acc[q, view] = product(u, q, False)
        elif op == "t":
            send0(u, q).wait_recv()
            s1[q, view] = (acc[q, view] + r0[q, view].astype(f32)).astype(bf16)
            send1(u, q).start()
        elif op == "t2":
            send0(u, 2).wait_recv()
            send1(u, 0).wait_recv()
            total = acc[2, view] + r0[2, view].astype(f32) + r1[0, view].astype(f32)
            s1[2, view] = total.astype(bf16)
            send1(u, 2).start()
        else:
            arrived = range(3) if kinds[u] == "D" else (1, 2)
            send0(u, 3).wait_recv()
            for k in arrived:
                send1(u, k).wait_recv()
            for part in range(2):
                some = pl.ds(2 * offsets[u] + part * sizes[u], sizes[u])
                total = acc[3, some] + r0[3, some].astype(f32)
                for k in arrived:
                    total = total + r1[k, some].astype(f32)
                out[part, rows] = total

    heard = 0
    for op, u, q in STEPS:
        if heard == 0 and op == "s":
            hear_two()
            heard = 1
        if heard == 1 and op in ("t", "t2"):
            hear_three()
            heard = 2
        step(op, u, q)

    for u in range(len(UNITS)):
        to_far(u).wait_send()
        to_last(u).wait_send()
        if u >= DIRECT:
            to_core(u).wait_send()
        for q in range(4):
            send0(u, q).wait_send()
        for k in range(3):
            send1(u, k).wait_send()


def kernel_body(n_ga, density, coulomb, row_block):
    local_g = density.shape[1]
    width = density.shape[2]
    own = width // n_ga
    flat = density.reshape(2 * local_g, width)
    window = -(-(RB + LANES - 1) // LANES) * LANES
    bf16, f32 = jnp.bfloat16, jnp.float32
    vmem, anywhere = pl.BlockSpec(memory_space=pltpu.VMEM), pl.BlockSpec(memory_space=pl.ANY)
    dma = pltpu.SemaphoreType.DMA
    masked = pl.pallas_call(
        functools.partial(pick_kernel, local_g, width, window),
        out_shape=jax.ShapeDtypeStruct((2, RB, local_g), bf16),
        in_specs=[pl.BlockSpec(memory_space=pltpu.SMEM), anywhere],
        out_specs=vmem,
        scratch_shapes=[pltpu.VMEM((2 * local_g, window), bf16), dma((2,))],
        compiler_params=pltpu.CompilerParams(vmem_limit_bytes=PICK_BYTES),
    )(row_block, flat)
    count = len(UNITS)
    kernel = pl.pallas_call(
        functools.partial(exchange_kernel, n_ga, local_g, own),
        out_shape=jax.ShapeDtypeStruct((2, RB, own), f32),
        in_specs=[vmem, vmem, anywhere],
        out_specs=vmem,
        scratch_shapes=[
            pltpu.VMEM((n_ga, 2 * local_g, own), bf16),
            pltpu.VMEM((2, RB, local_g), bf16),
            pltpu.VMEM((RB, local_g), bf16),
            pltpu.VMEM((2, RB, local_g), bf16),
            pltpu.VMEM((2, RB, local_g), bf16),
            pltpu.VMEM((2 * RB, 2 * local_g), bf16),
            pltpu.VMEM((4, 2 * RB, own), f32),
            pltpu.VMEM((4, 2 * RB, own), bf16),
            pltpu.VMEM((4, 2 * RB, own), bf16),
            pltpu.VMEM((3, 2 * RB, own), bf16),
            pltpu.VMEM((3, 2 * RB, own), bf16),
            dma((n_ga,)),
            dma((count,)), dma((count,)),
            dma((count,)), dma((count,)),
            dma((count,)), dma((count,)),
            dma((4 * count,)), dma((4 * count,)),
            dma((3 * count,)), dma((3 * count,)),
            pltpu.SemaphoreType.REGULAR, pltpu.SemaphoreType.REGULAR,
        ],
        compiler_params=pltpu.CompilerParams(
            collective_id=0, has_side_effects=True, vmem_limit_bytes=VMEM_BYTES
        ),
    )(masked, coulomb, flat)
    return jnp.transpose(kernel, (2, 0, 1))[None]


def solution(mesh):
    in_specs = (P(None, "ga", "ta"), P("ga"), P())
    out_specs = P("ta", "ga", None, None)
    n_ga, n_ta = mesh.shape["ga"], mesh.shape["ta"]

    def body(density, coulomb, row_block):
        _, local_g, width = density.shape
        aligned = local_g % LANES == 0 and width % (n_ga * LANES) == 0
        if aligned and n_ga == 8 and n_ta == 4:
            return kernel_body(n_ga, density, coulomb, row_block)
        return plain_body(density, coulomb, row_block)

    return jax.shard_map(body, mesh=mesh, in_specs=in_specs, out_specs=out_specs, check_vma=False)
```
